32 devices in a mesh: level: 2 (over x), row: 4 (over y, core), col: 4 (over z).
Axes of the slice: x: 2, y: 2, z: 4, core: 2. Of those that a mesh axis runs over, the one named last changes fastest.
Arguments:
- initial: float32 [3, 512, 4096], P(None, 'row', 'col'), may hold values from -0.75 to 0.75
Outputs:
- levels_out: float32 [2, 3, 512, 4096], P('level', None, 'row', 'col')
The draws below stay inside these ranges and needn't reach their ends.
All inputs are finite; a program needn't handle non-finite values.
Results may differ from the reference program's by a relative error of at most 0.00002.
Values sent between devices are 32-bit elements; how exact they have to be, the bound alone decides.
A program may use at most 64 MiB of HBM per device.

```python
import jax
import jax.numpy as jnp
from jax import lax

STEPS = 8
NX = 512
NY = 4096


def shard_levels(own_key, shape, split, smallest, top_value):
    def one(position, shards_of):
        draws = jax.random.uniform(jax.random.fold_in(jax.random.fold_in(own_key, 6), position), (shards_of,), jnp.float32, smallest / len(split), top_value / len(split))
        return jnp.repeat(jnp.exp(draws), shape[position] // shards_of).reshape((-1,) + (1,) * (len(shape) - position - 1))

    factor_of = one(*split[0])
    for cut in split[1:]:
        factor_of = factor_of * one(*cut)
    return factor_of


def centred(rng, shape, deviation, bound, pieces=(), held_as=jnp.bfloat16):
    entries = deviation * jax.random.normal(rng, shape, jnp.float32)
    if pieces:
        entries = entries * shard_levels(rng, shape, pieces, -0.22, 0.18)
    return jnp.clip(entries, -bound, bound).astype(held_as)


def setup_inputs(seed: int = 0) -> dict:
    key_list = jax.random.split(jax.random.key(seed), 2)
    return {
        "initial": centred(key_list[0], (3, NX, NY), 0.25, 0.75, ((1, 4), (2, 4)), jnp.float32),
    }


time_step = 0.1
gravity = 1.0
rotation = 0.2


def along_rows(values):
    return 0.5 * (jnp.roll(values, -1, axis=0) - jnp.roll(values, 1, axis=0))


def along_cols(values):
    return 0.5 * (jnp.roll(values, -1, axis=1) - jnp.roll(values, 1, axis=1))


def tendency(current):
    surface = current[0]
    eastward = current[1]
    northward = current[2]
    height = 1.0 + surface
    surface_rate = -(along_rows(height * eastward) + along_cols(height * northward))
    east_rate = -(eastward * along_rows(eastward) + northward * along_cols(eastward)) - gravity * along_rows(surface) + rotation * northward
    north_rate = -(eastward * along_rows(northward) + northward * along_cols(northward)) - gravity * along_cols(surface) - rotation * eastward
    return jnp.stack([surface_rate, east_rate, north_rate])


def reference(initial):
    def advance(moment, carry):
        predicted, corrected, predicted_rate = carry
        next_pred = predicted + time_step * predicted_rate
        next_rate = tendency(next_pred)
        corrected = corrected + time_step * tendency(corrected) + 0.5 * time_step * (next_rate - predicted_rate)
        return (next_pred, corrected, next_rate)

    start = initial.astype(jnp.float32)
    result = lax.fori_loop(0, STEPS, advance, (start, start, tendency(start)))
    return jnp.stack([result[0], result[1]])
```

```python
import functools

import jax
import jax.numpy as jnp
from jax import lax
from jax.experimental import pallas as pl
from jax.experimental.pallas import tpu as pltpu
from jax.sharding import PartitionSpec as P

STEPS = 8
time_step = 0.1
gravity = 1.0
rotation = 0.2

MESH = pl.DeviceIdType.MESH
LANES = 128
SUBS = 8
DEPTH = STEPS + 1
PACK = 16
TOP = 16

VEL = 0.5 * time_step
ELEV = VEL * VEL * gravity
TURN = time_step * rotation


def exchange(
    tile, rows, nine, cols, diag, top, bottom, edges, nine_out, pack, load_sem, send_sem, recv_sem
):
    fields, height, width = tile.shape
    n_row, n_col = lax.axis_size("row"), lax.axis_size("col")
    r, c = lax.axis_index("row"), lax.axis_index("col")
    up, down = lax.rem(r + n_row - 1, n_row), lax.rem(r + 1, n_row)
    left, right = lax.rem(c + n_col - 1, n_col), lax.rem(c + 1, n_col)
    loads = [
        pltpu.make_async_copy(tile.at[:, :, pl.ds(0, LANES)], edges.at[0], load_sem.at[0]),
        pltpu.make_async_copy(tile.at[:, :, pl.ds(width - LANES, LANES)], edges.at[1], load_sem.at[1]),
        pltpu.make_async_copy(tile.at[:, pl.ds(0, 16), :], top, load_sem.at[2]),
        pltpu.make_async_copy(tile.at[:, pl.ds(height - 16, 16), :], bottom, load_sem.at[3]),
    ]
    for load in loads:
        load.start()
    barrier = pltpu.get_barrier_semaphore()
    around = [(up, c), (down, c), (r, left), (r, right), (up, left), (up, right), (down, left), (down, right)]
    for to_r, to_c in around:
        pl.semaphore_signal(barrier, inc=1, device_id={"row": to_r, "col": to_c}, device_id_type=MESH)
    for load in loads:
        load.wait()
    tiles = width // LANES
    for f in range(fields):
        for t in range(tiles):
            nine_out[0, pl.ds(f * tiles + t, 1), :] = top[f, pl.ds(8, 1), pl.ds(t * LANES, LANES)]
            nine_out[1, pl.ds(f * tiles + t, 1), :] = bottom[f, pl.ds(7, 1), pl.ds(t * LANES, LANES)]
    lane_group = lax.broadcasted_iota(jnp.int32, (SUBS, LANES), 1) // PACK
    per = LANES // PACK
    for side in range(2):
        first = 0 if side == 0 else LANES - PACK
        for half in range(2):
            for f in range(fields):
                packed = None
                for g in range(per):
                    block = edges[side, f, pl.ds((half * per + g) * SUBS, SUBS), :]
                    amount = (g * PACK - first) % LANES
                    moved = pltpu.roll(block, amount, 1) if amount else block
                    packed = moved if packed is None else jnp.where(lane_group == g, moved, packed)
                pack[side, half, f] = packed
    pl.semaphore_wait(barrier, len(around))
    moves = [
        (top.at[:, pl.ds(0, 8), :], rows.at[1], up, c),
        (bottom.at[:, pl.ds(8, 8), :], rows.at[0], down, c),
        (pack.at[0, 0], diag.at[3], up, left),
        (pack.at[1, 0], diag.at[2], up, right),
        (pack.at[0, 1], diag.at[1], down, left),
        (pack.at[1, 1], diag.at[0], down, right),
        (pack.at[0], cols.at[1], r, left),
        (pack.at[1], cols.at[0], r, right),
        (nine_out.at[0], nine.at[1], up, c),
        (nine_out.at[1], nine.at[0], down, c),
    ]
    sends = [
        pltpu.make_async_remote_copy(
            src_ref=src,
            dst_ref=dst,
            send_sem=send_sem.at[i],
            recv_sem=recv_sem.at[i],
            device_id={"row": to_r, "col": to_c},
            device_id_type=MESH,
        )
        for i, (src, dst, to_r, to_c) in enumerate(moves)
    ]
    for send in sends:
        send.start()
    for send in sends:
        send.wait()


def call_exchange(initial):
    fields, height, width = initial.shape
    nine_rows = fields * width // LANES
    shape = functools.partial(jax.ShapeDtypeStruct, dtype=jnp.float32)
    vmem = lambda *dims: pltpu.VMEM(dims, jnp.float32)
    anywhere = pl.BlockSpec(memory_space=pl.ANY)
    return pl.pallas_call(
        exchange,
        out_shape=(
            shape((2, fields, 8, width)),
            shape((2, nine_rows, LANES)),
            shape((2, 2, fields, SUBS, LANES)),
            shape((4, fields, SUBS, LANES)),
        ),
        in_specs=[anywhere],
        out_specs=(anywhere,) * 4,
        scratch_shapes=[
            vmem(fields, 16, width),
            vmem(fields, 16, width),
            vmem(2, fields, height, LANES),
            vmem(2, nine_rows, LANES),
            vmem(2, 2, fields, SUBS, LANES),
            pltpu.SemaphoreType.DMA((4,)),
            pltpu.SemaphoreType.DMA((10,)),
            pltpu.SemaphoreType.DMA((10,)),
        ],
        compiler_params=pltpu.CompilerParams(
            collective_id=0, has_side_effects=True, vmem_limit_bytes=8 * 1024 * 1024
        ),
        name="exchange",
    )(initial)


def along_cols(x):
    return pltpu.roll(x, LANES - 1, 1) - pltpu.roll(x, 1, 1)


def full(state):
    e, u, v = state
    h = ELEV + e
    return e, u, v, h * u, h * v


def change(above, here, below):
    e0, u0, v0, hu0, _ = above
    e, u, v, _, hv = here
    e1, u1, v1, hu1, _ = below
    return (
        (hu1 - hu0) + along_cols(hv),
        u * (u1 - u0) + v * (along_cols(u) - TURN) + (e1 - e0),
        u * ((v1 - v0) + TURN) + v * along_cols(v) + along_cols(e),
    )


def row_of(ref, k):
    return tuple(ref[f, k] for f in range(3))


def put_row(ref, k, values):
    for f in range(3):
        ref[f, k] = values[f]


def from_above(state):
    return tuple(pltpu.roll(x, 1, 0) for x in state)


def from_below(state):
    return tuple(pltpu.roll(x, SUBS - 1, 0) for x in state)


def minus(state, rate):
    return tuple(a - b for a, b in zip(state, rate))


def minus_half(state, rate):
    return tuple(a - 0.5 * b for a, b in zip(state, rate))


def sweep(ref, use):
    count = ref.shape[1]
    above = full(from_above(row_of(ref, count - 1)))
    here = first = full(row_of(ref, 0))
    last = full(from_below(first[:3]))
    for k in range(count):
        below = last if k == count - 1 else full(row_of(ref, k + 1))
        use(k, here[:3], change(above, here, below))
        above, here = here, below


def predict(pred):
    sweep(pred, lambda k, state, rate: put_row(pred, k, minus(state, rate)))


def first_step(pred, base):
    def use(k, state, rate):
        put_row(pred, k, minus(state, rate))
        put_row(base, k, minus_half(state, rate))

    sweep(pred, use)


def middle_step(pred, base):
    count = pred.shape[1]
    corr = {}

    def correct(k, above, here, below):
        put_row(base, k, minus(row_of(base, k), change(above, here, below)))

    def use(k, state, rate):
        put_row(pred, k, minus(state, rate))
        corr[k] = full(minus_half(row_of(base, k), rate))
        if k >= 2:
            correct(k - 1, corr[k - 2], corr[k - 1], corr[k])

    sweep(pred, use)
    end = count - 1
    correct(end, corr[end - 1], corr[end], full(from_below(corr[0][:3])))
    correct(0, full(from_above(corr[end][:3])), corr[0], corr[1])


def last_step(pred, base):
    sweep(pred, lambda k, state, rate: put_row(pred, k, minus_half(row_of(base, k), rate)))


def strip_plan(width):
    for strips in range(width // LANES + 1, 4 * (width // LANES) + 4):
        for stride in range(-(-width // strips), LANES - 2 * DEPTH + 1):
            done = [min(width // LANES, stride * (t + 1) // LANES) for t in range(strips)]
            gaps = all(stride * t % LANES >= DEPTH for t in range(1, strips))
            if gaps and done[-1] == width // LANES and (strips - 1) * stride < width:
                return strips, stride


def window(
    tile, rows, nine, cols, diag, out, padded, result, pred, base, load_sem, halo_sem, out_sem
):
    fields, height, width = tile.shape
    tiles = width // LANES
    count = pred.shape[1]
    strips, stride = strip_plan(width)
    level = lax.axis_index("level")
    loads = []
    for j in range(tiles):
        lanes = pl.ds(j * LANES, LANES)
        loads += [
            pltpu.make_async_copy(
                tile.at[:, :, lanes], padded.at[:, j + 1, pl.ds(TOP, height), :], load_sem.at[j]
            ),
            pltpu.make_async_copy(
                rows.at[0, :, :, lanes], padded.at[:, j + 1, pl.ds(TOP - 8, 8), :], halo_sem.at[0, j]
            ),
            pltpu.make_async_copy(
                rows.at[1, :, :, lanes], padded.at[:, j + 1, pl.ds(TOP + height, 8), :], halo_sem.at[1, j]
            ),
        ]
    for load in loads:
        load.start()
    per = LANES // PACK

    def unpack(side, f, at, block, g):
        amount = ((LANES - PACK if side == 0 else 0) - g * PACK) % LANES
        moved = pltpu.roll(block, amount, 1) if amount else block
        padded[f, 0 if side == 0 else tiles + 1, pl.ds(at, SUBS), :] = moved

    for side in range(2):
        for f in range(fields):
            for half in range(2):
                block = cols[side, half, f]
                for g in range(per):
                    unpack(side, f, TOP + (half * per + g) * SUBS, block, g)
            for i in range(2):
                unpack(side, f, TOP - 16 + i * SUBS, diag[side, f], per - 2 + i)
                unpack(side, f, TOP + height + i * SUBS, diag[2 + side, f], i)
    for f in range(fields):
        for j in range(tiles):
            padded[f, j + 1, pl.ds(TOP - DEPTH, 1), :] = nine[0, pl.ds(f * tiles + j, 1), :]
            padded[f, j + 1, pl.ds(TOP + height + DEPTH - 1, 1), :] = nine[1, pl.ds(f * tiles + j, 1), :]
    for load in loads:
        load.wait()

    lane = lax.broadcasted_iota(jnp.int32, (SUBS, LANES), 1)
    into = (ELEV, VEL, VEL)

    def out_copy(j):
        return pltpu.make_async_copy(
            result.at[:, j + 1, pl.ds(TOP, height), :],
            out.at[0, :, :, pl.ds(pl.multiple_of(j * LANES, LANES), LANES)],
            out_sem.at[j],
        )

    def strip(t, carry):
        start = t * stride + LANES - DEPTH
        a = start // LANES
        offset = start - a * LANES
        from_first = lane >= offset
        for f in range(fields):
            for k in range(count):
                at = pl.ds(TOP - DEPTH + k, SUBS, stride=count)
                both = jnp.where(from_first, padded[f, a, at, :], padded[f, a + 1, at, :])
                pred[f, k] = into[f] * pltpu.roll(both, LANES - offset, 1)

        @pl.when(level == 0)
        def _():
            lax.fori_loop(0, STEPS, lambda m, x: (predict(pred), x)[1], 0)

        @pl.when(level == 1)
        def _():
            first_step(pred, base)
            lax.fori_loop(1, STEPS, lambda m, x: (middle_step(pred, base), x)[1], 0)
            last_step(pred, base)

        source = jnp.where(from_first, lane - offset, lane - offset + LANES)
        inside = (source >= DEPTH) & (source < DEPTH + stride)
        low, high = from_first & inside, jnp.logical_not(from_first) & inside
        for f in range(fields):
            for k in range(count):
                at = pl.ds(TOP - DEPTH + k, SUBS, stride=count)
                moved = pltpu.roll((1.0 / into[f]) * pred[f, k], offset, 1)
                result[f, a, at, :] = jnp.where(low, moved, result[f, a, at, :])
                result[f, a + 1, at, :] = jnp.where(high, moved, result[f, a + 1, at, :])
        done = jnp.minimum(tiles, (t + 1) * stride // LANES)
        before = jnp.minimum(tiles, t * stride // LANES)

        @pl.when(done > before)
        def _():
            out_copy(done - 1).start()

        return carry

    lax.fori_loop(0, strips, strip, 0)
    for j in range(tiles):
        out_copy(j).wait()


def call_window(initial, rows, nine, cols, diag):
    fields, height, width = initial.shape
    tiles = width // LANES
    count = -(-(height + 2 * DEPTH) // SUBS)
    padded_rows = height + 2 * TOP
    vmem = lambda *dims: pltpu.VMEM(dims, jnp.float32)
    anywhere = pl.BlockSpec(memory_space=pl.ANY)
    local = pl.BlockSpec(memory_space=pltpu.VMEM)
    return pl.pallas_call(
        window,
        out_shape=jax.ShapeDtypeStruct((1, fields, height, width), jnp.float32),
        in_specs=[anywhere, anywhere, local, local, local],
        out_specs=anywhere,
        scratch_shapes=[
            vmem(fields, tiles + 2, padded_rows, LANES),
            vmem(fields, tiles + 2, padded_rows, LANES),
            vmem(fields, count, SUBS, LANES),
            vmem(fields, count, SUBS, LANES),
            pltpu.SemaphoreType.DMA((tiles,)),
            pltpu.SemaphoreType.DMA((2, tiles)),
            pltpu.SemaphoreType.DMA((tiles,)),
        ],
        compiler_params=pltpu.CompilerParams(vmem_limit_bytes=16 * 1024 * 1024),
        name="window",
    )(initial, rows, nine, cols, diag)


def body(initial):
    return call_window(initial, *call_exchange(initial))


def solution(mesh):
    return jax.shard_map(
        body,
        mesh=mesh,
        in_specs=(P(None, "row", "col"),),
        out_specs=P("level", None, "row", "col"),
        check_vma=False,
    )
```

```python
import functools

import jax
import jax.numpy as jnp
from jax import lax
from jax.experimental import pallas as pl
from jax.experimental.pallas import tpu as pltpu
from jax.sharding import PartitionSpec as P

STEPS = 8
time_step = 0.1
gravity = 1.0
rotation = 0.2

MESH = pl.DeviceIdType.MESH
LANES = 128
SUBS = 8
DEPTH = STEPS + 1
PACK = 16
TOP = 16

VEL = 0.5 * time_step
ELEV = VEL * VEL * gravity
TURN = time_step * rotation


def exchange(
    tile, rows, nine, cols, diag, top, bottom, edges, nine_out, pack, load_sem, send_sem, recv_sem
):
    fields, height, width = tile.shape
    n_row, n_col = lax.axis_size("row"), lax.axis_size("col")
    r, c = lax.axis_index("row"), lax.axis_index("col")
    up, down = lax.rem(r + n_row - 1, n_row), lax.rem(r + 1, n_row)
    left, right = lax.rem(c + n_col - 1, n_col), lax.rem(c + 1, n_col)
    loads = [
        pltpu.make_async_copy(tile.at[:, :, pl.ds(0, LANES)], edges.at[0], load_sem.at[0]),
        pltpu.make_async_copy(tile.at[:, :, pl.ds(width - LANES, LANES)], edges.at[1], load_sem.at[1]),
        pltpu.make_async_copy(tile.at[:, pl.ds(0, 16), :], top, load_sem.at[2]),
        pltpu.make_async_copy(tile.at[:, pl.ds(height - 16, 16), :], bottom, load_sem.at[3]),
    ]
    for load in loads:
        load.start()
    barrier = pltpu.get_barrier_semaphore()
    around = [(up, c), (down, c), (r, left), (r, right), (up, left), (up, right), (down, left), (down, right)]
    for to_r, to_c in around:
        pl.semaphore_signal(barrier, inc=1, device_id={"row": to_r, "col": to_c}, device_id_type=MESH)
    for load in loads:
        load.wait()
    tiles = width // LANES
    for f in range(fields):
        for t in range(tiles):
            nine_out[0, pl.ds(f * tiles + t, 1), :] = top[f, pl.ds(8, 1), pl.ds(t * LANES, LANES)]
            nine_out[1, pl.ds(f * tiles + t, 1), :] = bottom[f, pl.ds(7, 1), pl.ds(t * LANES, LANES)]
    lane_group = lax.broadcasted_iota(jnp.int32, (SUBS, LANES), 1) // PACK
    per = LANES // PACK
    for side in range(2):
        first = 0 if side == 0 else LANES - PACK
        for half in range(2):
            for f in range(fields):
                packed = None
                for g in range(per):
                    block = edges[side, f, pl.ds((half * per + g) * SUBS, SUBS), :]
                    amount = (g * PACK - first) % LANES
                    moved = pltpu.roll(block, amount, 1) if amount else block
                    packed = moved if packed is None else jnp.where(lane_group == g, moved, packed)
                pack[side, half, f] = packed
    pl.semaphore_wait(barrier, len(around))
    moves = [
        (top.at[:, pl.ds(0, 8), :], rows.at[1], up, c),
        (bottom.at[:, pl.ds(8, 8), :], rows.at[0], down, c),
        (pack.at[0, 0], diag.at[3], up, left),
        (pack.at[1, 0], diag.at[2], up, right),
        (pack.at[0, 1], diag.at[1], down, left),
        (pack.at[1, 1], diag.at[0], down, right),
        (pack.at[0], cols.at[1], r, left),
        (pack.at[1], cols.at[0], r, right),
        (nine_out.at[0], nine.at[1], up, c),
        (nine_out.at[1], nine.at[0], down, c),
    ]
    sends = [
        pltpu.make_async_remote_copy(
            src_ref=src,
            dst_ref=dst,
            send_sem=send_sem.at[i],
            recv_sem=recv_sem.at[i],
            device_id={"row": to_r, "col": to_c},
            device_id_type=MESH,
        )
        for i, (src, dst, to_r, to_c) in enumerate(moves)
    ]
    for send in sends:
        send.start()
    for send in sends:
        send.wait()


def call_exchange(initial):
    fields, height, width = initial.shape
    nine_rows = fields * width // LANES
    shape = functools.partial(jax.ShapeDtypeStruct, dtype=jnp.float32)
    vmem = lambda *dims: pltpu.VMEM(dims, jnp.float32)
    anywhere = pl.BlockSpec(memory_space=pl.ANY)
    return pl.pallas_call(
        exchange,
        out_shape=(
            shape((2, fields, 8, width)),
            shape((2, nine_rows, LANES)),
            shape((2, 2, fields, SUBS, LANES)),
            shape((4, fields, SUBS, LANES)),
        ),
        in_specs=[anywhere],
        out_specs=(anywhere,) * 4,
        scratch_shapes=[
            vmem(fields, 16, width),
            vmem(fields, 16, width),
            vmem(2, fields, height, LANES),
            vmem(2, nine_rows, LANES),
            vmem(2, 2, fields, SUBS, LANES),
            pltpu.SemaphoreType.DMA((4,)),
            pltpu.SemaphoreType.DMA((10,)),
            pltpu.SemaphoreType.DMA((10,)),
        ],
        compiler_params=pltpu.CompilerParams(
            collective_id=0, has_side_effects=True, vmem_limit_bytes=8 * 1024 * 1024
        ),
        name="exchange",
    )(initial)


def along_cols(x):
    return pltpu.roll(x, LANES - 1, 1) - pltpu.roll(x, 1, 1)


def full(state):
    e, u, v = state
    h = ELEV + e
    return e, u, v, h * u, h * v


def change(above, here, below, slopes):
    e0, u0, v0, hu0, _ = above
    e, u, v, _, hv = here
    e1, u1, v1, hu1, _ = below
    along_e, along_u, along_v = slopes
    return (
        (hu1 - hu0) + along_cols(hv),
        u * (u1 - u0) + v * (along_u - TURN) + (e1 - e0),
        u * ((v1 - v0) + TURN) + v * along_v + along_e,
    )


def row_of(ref, k):
    return tuple(ref[f, k] for f in range(3))


def put_row(ref, k, values):
    for f in range(3):
        ref[f, k] = values[f]


def from_above(state):
    return tuple(pltpu.roll(x, 1, 0) for x in state)


def from_below(state):
    return tuple(pltpu.roll(x, SUBS - 1, 0) for x in state)


def minus(state, rate):
    return tuple(a - b for a, b in zip(state, rate))


def minus_half(state, rate):
    return tuple(a - 0.5 * b for a, b in zip(state, rate))


def band():
    source = lax.broadcasted_iota(jnp.int32, (2 * LANES, LANES), 0) % LANES
    target = lax.broadcasted_iota(jnp.int32, (2 * LANES, LANES), 1)
    ahead = jnp.where(source == target + 1, 1.0, 0.0)
    return (ahead - jnp.where(source == target - 1, 1.0, 0.0)).astype(jnp.bfloat16)


def put_slopes(matrix, places):
    values = jnp.concatenate([x for _, _, state in places for x in state], axis=0)
    main = values.astype(jnp.bfloat16)
    rest = (values - main.astype(jnp.float32)).astype(jnp.bfloat16)
    out = jnp.dot(
        jnp.concatenate([main, rest], axis=1), matrix[...], preferred_element_type=jnp.float32
    )
    for i, (ref, k, _) in enumerate(places):
        for f in range(3):
            at = (3 * i + f) * SUBS
            ref[f, k] = out[at : at + SUBS]


CHUNK = 5


def chunk_ends(count):
    return [min(k + CHUNK, count) for k in range(0, count, CHUNK)]


def sweep(ref, slope, use):
    count = ref.shape[1]
    above = full(from_above(row_of(ref, count - 1)))
    here = first = full(row_of(ref, 0))
    last = full(from_below(first[:3]))
    for k in range(count):
        below = last if k == count - 1 else full(row_of(ref, k + 1))
        use(k, here[:3], change(above, here, below, row_of(slope, k)))
        above, here = here, below


def stepping(pred, pred_slope, matrix, each):
    ends = chunk_ends(pred.shape[1])
    places = []

    def use(k, state, rate):
        after = minus(state, rate)
        put_row(pred, k, after)
        places.append((pred_slope, k, after))
        places.extend(each(k, state, rate))
        if k + 1 in ends:
            put_slopes(matrix, places)
            places.clear()

    sweep(pred, pred_slope, use)


def predict(pred, pred_slope, matrix):
    stepping(pred, pred_slope, matrix, lambda k, state, rate: [])


def first_step(pred, pred_slope, matrix, base):
    def each(k, state, rate):
        put_row(base, k, minus_half(state, rate))
        return []

    stepping(pred, pred_slope, matrix, each)


def middle_step(pred, pred_slope, matrix, base, corr, corr_slope):
    count = pred.shape[1]
    held = {}

    def correct(upto):
        if "next" not in held:
            held["next"], held["above"], held["here"] = 1, full(row_of(corr, 0)), full(row_of(corr, 1))
        while held["next"] < upto:
            k = held["next"]
            if k == count - 1:
                below = full(from_below(row_of(corr, 0)))
            else:
                below = full(row_of(corr, k + 1))
            rate = change(held["above"], held["here"], below, row_of(corr_slope, k))
            put_row(base, k, minus(row_of(base, k), rate))
            held["next"], held["above"], held["here"] = k + 1, held["here"], below

    def each(k, state, rate):
        value = minus_half(row_of(base, k), rate)
        put_row(corr, k, value)
        if k >= 2 * CHUNK:
            correct(k - 2 * CHUNK + 2)
        return [(corr_slope, k, value)]

    stepping(pred, pred_slope, matrix, each)
    correct(count)
    above = full(from_above(row_of(corr, count - 1)))
    rate = change(above, full(row_of(corr, 0)), full(row_of(corr, 1)), row_of(corr_slope, 0))
    put_row(base, 0, minus(row_of(base, 0), rate))


def last_step(pred, pred_slope, base):
    sweep(pred, pred_slope, lambda k, state, rate: put_row(pred, k, minus_half(row_of(base, k), rate)))


def strip_plan(width):
    for strips in range(width // LANES + 1, 4 * (width // LANES) + 4):
        for stride in range(-(-width // strips), LANES - 2 * DEPTH + 1):
            done = [min(width // LANES, stride * (t + 1) // LANES) for t in range(strips)]
            gaps = all(stride * t % LANES >= DEPTH for t in range(1, strips))
            if gaps and done[-1] == width // LANES and (strips - 1) * stride < width:
                return strips, stride


def window(
    tile, rows, nine, cols, diag, out, padded, result, pred, base, corr, pred_slope, corr_slope, matrix,
    load_sem, halo_sem, out_sem
):
    fields, height, width = tile.shape
    tiles = width // LANES
    count = pred.shape[1]
    strips, stride = strip_plan(width)
    level = lax.axis_index("level")
    loads = []
    for j in range(tiles):
        lanes = pl.ds(j * LANES, LANES)
        loads += [
            pltpu.make_async_copy(
                tile.at[:, :, lanes], padded.at[:, j + 1, pl.ds(TOP, height), :], load_sem.at[j]
            ),
            pltpu.make_async_copy(
                rows.at[0, :, :, lanes], padded.at[:, j + 1, pl.ds(TOP - 8, 8), :], halo_sem.at[0, j]
            ),
            pltpu.make_async_copy(
                rows.at[1, :, :, lanes], padded.at[:, j + 1, pl.ds(TOP + height, 8), :], halo_sem.at[1, j]
            ),
        ]
    for load in loads:
        load.start()
    per = LANES // PACK

    def unpack(side, f, at, block, g):
        amount = ((LANES - PACK if side == 0 else 0) - g * PACK) % LANES
        moved = pltpu.roll(block, amount, 1) if amount else block
        padded[f, 0 if side == 0 else tiles + 1, pl.ds(at, SUBS), :] = moved

    for side in range(2):
        for f in range(fields):
            for half in range(2):
                block = cols[side, half, f]
                for g in range(per):
                    unpack(side, f, TOP + (half * per + g) * SUBS, block, g)
            for i in range(2):
                unpack(side, f, TOP - 16 + i * SUBS, diag[side, f], per - 2 + i)
                unpack(side, f, TOP + height + i * SUBS, diag[2 + side, f], i)
    for f in range(fields):
        for j in range(tiles):
            padded[f, j + 1, pl.ds(TOP - DEPTH, 1), :] = nine[0, pl.ds(f * tiles + j, 1), :]
            padded[f, j + 1, pl.ds(TOP + height + DEPTH - 1, 1), :] = nine[1, pl.ds(f * tiles + j, 1), :]
    for load in loads:
        load.wait()

    matrix[...] = band()
    lane = lax.broadcasted_iota(jnp.int32, (SUBS, LANES), 1)
    into = (ELEV, VEL, VEL)

    def out_copy(j):
        return pltpu.make_async_copy(
            result.at[:, j + 1, pl.ds(TOP, height), :],
            out.at[0, :, :, pl.ds(pl.multiple_of(j * LANES, LANES), LANES)],
            out_sem.at[j],
        )

    def strip(t, carry):
        start = t * stride + LANES - DEPTH
        a = start // LANES
        offset = start - a * LANES
        from_first = lane >= offset
        places = []
        for k in range(count):
            at = pl.ds(TOP - DEPTH + k, SUBS, stride=count)
            state = ()
            for f in range(fields):
                both = jnp.where(from_first, padded[f, a, at, :], padded[f, a + 1, at, :])
                state += (into[f] * pltpu.roll(both, LANES - offset, 1),)
            put_row(pred, k, state)
            places.append((pred_slope, k, state))
        put_slopes(matrix, places)

        @pl.when(level == 0)
        def _():
            lax.fori_loop(0, STEPS, lambda m, x: (predict(pred, pred_slope, matrix), x)[1], 0)

        @pl.when(level == 1)
        def _():
            first_step(pred, pred_slope, matrix, base)

            def middle(m, x):
                middle_step(pred, pred_slope, matrix, base, corr, corr_slope)
                return x

            lax.fori_loop(1, STEPS, middle, 0)
            last_step(pred, pred_slope, base)

        source = jnp.where(from_first, lane - offset, lane - offset + LANES)
        inside = (source >= DEPTH) & (source < DEPTH + stride)
        low, high = from_first & inside, jnp.logical_not(from_first) & inside
        for f in range(fields):
            for k in range(count):
                at = pl.ds(TOP - DEPTH + k, SUBS, stride=count)
                moved = pltpu.roll((1.0 / into[f]) * pred[f, k], offset, 1)
                result[f, a, at, :] = jnp.where(low, moved, result[f, a, at, :])
                result[f, a + 1, at, :] = jnp.where(high, moved, result[f, a + 1, at, :])
        done = jnp.minimum(tiles, (t + 1) * stride // LANES)
        before = jnp.minimum(tiles, t * stride // LANES)

        @pl.when(done > before)
        def _():
            out_copy(done - 1).start()

        return carry

    lax.fori_loop(0, strips, strip, 0)
    for j in range(tiles):
        out_copy(j).wait()


def call_window(initial, rows, nine, cols, diag):
    fields, height, width = initial.shape
    tiles = width // LANES
    count = -(-(height + 2 * DEPTH) // SUBS)
    padded_rows = height + 2 * TOP
    vmem = lambda *dims: pltpu.VMEM(dims, jnp.float32)
    anywhere = pl.BlockSpec(memory_space=pl.ANY)
    local = pl.BlockSpec(memory_space=pltpu.VMEM)
    return pl.pallas_call(
        window,
        out_shape=jax.ShapeDtypeStruct((1, fields, height, width), jnp.float32),
        in_specs=[anywhere, anywhere, local, local, local],
        out_specs=anywhere,
        scratch_shapes=[
            vmem(fields, tiles + 2, padded_rows, LANES),
            vmem(fields, tiles + 2, padded_rows, LANES),
            vmem(fields, count, SUBS, LANES),
            vmem(fields, count, SUBS, LANES),
            vmem(fields, count, SUBS, LANES),
            vmem(fields, count, SUBS, LANES),
            vmem(fields, count, SUBS, LANES),
            pltpu.VMEM((2 * LANES, LANES), jnp.bfloat16),
            pltpu.SemaphoreType.DMA((tiles,)),
            pltpu.SemaphoreType.DMA((2, tiles)),
            pltpu.SemaphoreType.DMA((tiles,)),
        ],
        compiler_params=pltpu.CompilerParams(vmem_limit_bytes=16 * 1024 * 1024),
        name="window",
    )(initial, rows, nine, cols, diag)


def body(initial):
    return call_window(initial, *call_exchange(initial))


def solution(mesh):
    return jax.shard_map(
        body,
        mesh=mesh,
        in_specs=(P(None, "row", "col"),),
        out_specs=P("level", None, "row", "col"),
        check_vma=False,
    )
```

```python
import functools

import jax
import jax.numpy as jnp
from jax import lax
from jax.experimental import pallas as pl
from jax.experimental.pallas import tpu as pltpu
from jax.sharding import PartitionSpec as P

STEPS = 8
time_step = 0.1
gravity = 1.0
rotation = 0.2

MESH = pl.DeviceIdType.MESH
LANES = 128
SUBS = 8
DEPTH = STEPS + 1
PACK = 16
TOP = 16

VEL = 0.5 * time_step
ELEV = VEL * VEL * gravity
TURN = time_step * rotation


def exchange(
    tile, rows, nine, cols, diag, top, bottom, edges, nine_out, pack, load_sem, send_sem, recv_sem
):
    fields, height, width = tile.shape
    n_row, n_col = lax.axis_size("row"), lax.axis_size("col")
    r, c = lax.axis_index("row"), lax.axis_index("col")
    up, down = lax.rem(r + n_row - 1, n_row), lax.rem(r + 1, n_row)
    left, right = lax.rem(c + n_col - 1, n_col), lax.rem(c + 1, n_col)
    loads = [
        pltpu.make_async_copy(tile.at[:, :, pl.ds(0, LANES)], edges.at[0], load_sem.at[0]),
        pltpu.make_async_copy(tile.at[:, :, pl.ds(width - LANES, LANES)], edges.at[1], load_sem.at[1]),
        pltpu.make_async_copy(tile.at[:, pl.ds(0, 16), :], top, load_sem.at[2]),
        pltpu.make_async_copy(tile.at[:, pl.ds(height - 16, 16), :], bottom, load_sem.at[3]),
    ]
    for load in loads:
        load.start()
    barrier = pltpu.get_barrier_semaphore()
    around = [(up, c), (down, c), (r, left), (r, right), (up, left), (up, right), (down, left), (down, right)]
    for to_r, to_c in around:
        pl.semaphore_signal(barrier, inc=1, device_id={"row": to_r, "col": to_c}, device_id_type=MESH)
    for load in loads:
        load.wait()
    tiles = width // LANES
    for f in range(fields):
        for t in range(tiles):
            nine_out[0, pl.ds(f * tiles + t, 1), :] = top[f, pl.ds(8, 1), pl.ds(t * LANES, LANES)]
            nine_out[1, pl.ds(f * tiles + t, 1), :] = bottom[f, pl.ds(7, 1), pl.ds(t * LANES, LANES)]
    lane_group = lax.broadcasted_iota(jnp.int32, (SUBS, LANES), 1) // PACK
    per = LANES // PACK
    for side in range(2):
        first = 0 if side == 0 else LANES - PACK
        for half in range(2):
            for f in range(fields):
                packed = None
                for g in range(per):
                    block = edges[side, f, pl.ds((half * per + g) * SUBS, SUBS), :]
                    amount = (g * PACK - first) % LANES
                    moved = pltpu.roll(block, amount, 1) if amount else block
                    packed = moved if packed is None else jnp.where(lane_group == g, moved, packed)
                pack[side, half, f] = packed
    pl.semaphore_wait(barrier, len(around))
    moves = [
        (top.at[:, pl.ds(0, 8), :], rows.at[1], up, c),
        (bottom.at[:, pl.ds(8, 8), :], rows.at[0], down, c),
        (pack.at[0, 0], diag.at[3], up, left),
        (pack.at[1, 0], diag.at[2], up, right),
        (pack.at[0, 1], diag.at[1], down, left),
        (pack.at[1, 1], diag.at[0], down, right),
        (pack.at[0], cols.at[1], r, left),
        (pack.at[1], cols.at[0], r, right),
        (nine_out.at[0], nine.at[1], up, c),
        (nine_out.at[1], nine.at[0], down, c),
    ]
    sends = [
        pltpu.make_async_remote_copy(
            src_ref=src,
            dst_ref=dst,
            send_sem=send_sem.at[i],
            recv_sem=recv_sem.at[i],
            device_id={"row": to_r, "col": to_c},
            device_id_type=MESH,
        )
        for i, (src, dst, to_r, to_c) in enumerate(moves)
    ]
    for send in sends:
        send.start()
    for send in sends:
        send.wait()


def call_exchange(initial):
    fields, height, width = initial.shape
    nine_rows = fields * width // LANES
    shape = functools.partial(jax.ShapeDtypeStruct, dtype=jnp.float32)
    vmem = lambda *dims: pltpu.VMEM(dims, jnp.float32)
    anywhere = pl.BlockSpec(memory_space=pl.ANY)
    return pl.pallas_call(
        exchange,
        out_shape=(
            shape((2, fields, 8, width)),
            shape((2, nine_rows, LANES)),
            shape((2, 2, fields, SUBS, LANES)),
            shape((4, fields, SUBS, LANES)),
        ),
        in_specs=[anywhere],
        out_specs=(anywhere,) * 4,
        scratch_shapes=[
            vmem(fields, 16, width),
            vmem(fields, 16, width),
            vmem(2, fields, height, LANES),
            vmem(2, nine_rows, LANES),
            vmem(2, 2, fields, SUBS, LANES),
            pltpu.SemaphoreType.DMA((4,)),
            pltpu.SemaphoreType.DMA((10,)),
            pltpu.SemaphoreType.DMA((10,)),
        ],
        compiler_params=pltpu.CompilerParams(
            collective_id=0, has_side_effects=True, vmem_limit_bytes=65994752
        ),
        name="exchange",
    )(initial)


def along_cols(x):
    return pltpu.roll(x, LANES - 1, 1) - pltpu.roll(x, 1, 1)


def full(state):
    e, u, v = state
    h = ELEV + e
    return e, u, v, h * u, h * v


def change(above, here, below, slopes):
    e0, u0, v0, hu0, _ = above
    e, u, v, _, hv = here
    e1, u1, v1, hu1, _ = below
    along_e, along_u, along_v = slopes
    return (
        (hu1 - hu0) + along_cols(hv),
        u * (u1 - u0) + v * (along_u - TURN) + (e1 - e0),
        u * ((v1 - v0) + TURN) + v * along_v + along_e,
    )


def row_of(ref, k):
    return tuple(ref[f, k] for f in range(3))


def put_row(ref, k, values):
    for f in range(3):
        ref[f, k] = values[f]


def from_above(state):
    return tuple(pltpu.roll(x, 1, 0) for x in state)


def from_below(state):
    return tuple(pltpu.roll(x, SUBS - 1, 0) for x in state)


def minus(state, rate):
    return tuple(a - b for a, b in zip(state, rate))


def minus_half(state, rate):
    return tuple(a - 0.5 * b for a, b in zip(state, rate))


def band():
    source = lax.broadcasted_iota(jnp.int32, (2 * LANES, LANES), 0) % LANES
    target = lax.broadcasted_iota(jnp.int32, (2 * LANES, LANES), 1)
    ahead = jnp.where(source == target + 1, 1.0, 0.0)
    return (ahead - jnp.where(source == target - 1, 1.0, 0.0)).astype(jnp.bfloat16)


def put_slopes(matrix, places):
    values = jnp.concatenate([x for _, _, state in places for x in state], axis=0)
    main = values.astype(jnp.bfloat16)
    rest = (values - main.astype(jnp.float32)).astype(jnp.bfloat16)
    out = jnp.dot(
        jnp.concatenate([main, rest], axis=1), matrix[...], preferred_element_type=jnp.float32
    )
    for i, (ref, k, _) in enumerate(places):
        for f in range(3):
            at = (3 * i + f) * SUBS
            ref[f, k] = out[at : at + SUBS]


CHUNK = 19


def chunk_ends(count):
    return [min(k + CHUNK, count) for k in range(0, count, CHUNK)]


def sweep(ref, slope, use):
    count = ref.shape[1]
    above = full(from_above(row_of(ref, count - 1)))
    here = first = full(row_of(ref, 0))
    last = full(from_below(first[:3]))
    for k in range(count):
        below = last if k == count - 1 else full(row_of(ref, k + 1))
        use(k, here[:3], change(above, here, below, row_of(slope, k)))
        above, here = here, below


def stepping(pred, pred_slope, matrix, each):
    ends = chunk_ends(pred.shape[1])
    places = []

    def use(k, state, rate):
        after = minus(state, rate)
        put_row(pred, k, after)
        places.append((pred_slope, k, after))
        places.extend(each(k, state, rate))
        if k + 1 in ends:
            put_slopes(matrix, places)
            places.clear()

    sweep(pred, pred_slope, use)


def predict(pred, pred_slope, matrix):
    stepping(pred, pred_slope, matrix, lambda k, state, rate: [])


def first_step(pred, pred_slope, matrix, base):
    def each(k, state, rate):
        put_row(base, k, minus_half(state, rate))
        return []

    stepping(pred, pred_slope, matrix, each)


def middle_step(pred, pred_slope, matrix, base, corr, corr_slope):
    count = pred.shape[1]
    held = {}

    def correct(upto):
        if "next" not in held:
            held["next"], held["above"], held["here"] = 1, full(row_of(corr, 0)), full(row_of(corr, 1))
        while held["next"] < upto:
            k = held["next"]
            if k == count - 1:
                below = full(from_below(row_of(corr, 0)))
            else:
                below = full(row_of(corr, k + 1))
            rate = change(held["above"], held["here"], below, row_of(corr_slope, k))
            put_row(base, k, minus(row_of(base, k), rate))
            held["next"], held["above"], held["here"] = k + 1, held["here"], below

    def each(k, state, rate):
        value = minus_half(row_of(base, k), rate)
        put_row(corr, k, value)
        if k >= 2 * CHUNK:
            correct(k - 2 * CHUNK + 2)
        return [(corr_slope, k, value)]

    stepping(pred, pred_slope, matrix, each)
    correct(count)
    above = full(from_above(row_of(corr, count - 1)))
    rate = change(above, full(row_of(corr, 0)), full(row_of(corr, 1)), row_of(corr_slope, 0))
    put_row(base, 0, minus(row_of(base, 0), rate))


def last_step(pred, pred_slope, base):
    sweep(pred, pred_slope, lambda k, state, rate: put_row(pred, k, minus_half(row_of(base, k), rate)))


def strip_plan(width):
    for strips in range(width // LANES + 1, 4 * (width // LANES) + 4):
        for stride in range(-(-width // strips), LANES - 2 * DEPTH + 1):
            done = [min(width // LANES, stride * (t + 1) // LANES) for t in range(strips)]
            gaps = all(stride * t % LANES >= DEPTH for t in range(1, strips))
            if gaps and done[-1] == width // LANES and (strips - 1) * stride < width:
                return strips, stride


def window(
    tile, rows, nine, cols, diag, out, padded, result, pred, base, corr, pred_slope, corr_slope, matrix,
    load_sem, halo_sem, out_sem
):
    fields, height, width = tile.shape
    tiles = width // LANES
    count = pred.shape[1]
    strips, stride = strip_plan(width)
    level = lax.axis_index("level")
    loads = []
    for j in range(tiles):
        lanes = pl.ds(j * LANES, LANES)
        loads += [
            pltpu.make_async_copy(
                tile.at[:, :, lanes], padded.at[:, j + 1, pl.ds(TOP, height), :], load_sem.at[j]
            ),
            pltpu.make_async_copy(
                rows.at[0, :, :, lanes], padded.at[:, j + 1, pl.ds(TOP - 8, 8), :], halo_sem.at[0, j]
            ),
            pltpu.make_async_copy(
                rows.at[1, :, :, lanes], padded.at[:, j + 1, pl.ds(TOP + height, 8), :], halo_sem.at[1, j]
            ),
        ]
    for load in loads:
        load.start()
    per = LANES // PACK

    def unpack(side, f, at, block, g):
        amount = ((LANES - PACK if side == 0 else 0) - g * PACK) % LANES
        moved = pltpu.roll(block, amount, 1) if amount else block
        padded[f, 0 if side == 0 else tiles + 1, pl.ds(at, SUBS), :] = moved

    for side in range(2):
        for f in range(fields):
            for half in range(2):
                block = cols[side, half, f]
                for g in range(per):
                    unpack(side, f, TOP + (half * per + g) * SUBS, block, g)
            for i in range(2):
                unpack(side, f, TOP - 16 + i * SUBS, diag[side, f], per - 2 + i)
                unpack(side, f, TOP + height + i * SUBS, diag[2 + side, f], i)
    for f in range(fields):
        for j in range(tiles):
            padded[f, j + 1, pl.ds(TOP - DEPTH, 1), :] = nine[0, pl.ds(f * tiles + j, 1), :]
            padded[f, j + 1, pl.ds(TOP + height + DEPTH - 1, 1), :] = nine[1, pl.ds(f * tiles + j, 1), :]
    def await_tile(j):
        pltpu.make_async_copy(
            tile.at[:, :, pl.ds(0, LANES)], padded.at[:, j + 1, pl.ds(TOP, height), :], load_sem.at[j]
        ).wait()
        for side, at in ((0, TOP - 8), (1, TOP + height)):
            pltpu.make_async_copy(
                rows.at[side, :, :, pl.ds(0, LANES)],
                padded.at[:, j + 1, pl.ds(at, 8), :],
                halo_sem.at[side, j],
            ).wait()

    matrix[...] = band()
    lane = lax.broadcasted_iota(jnp.int32, (SUBS, LANES), 1)
    into = (ELEV, VEL, VEL)

    def out_copy(j):
        return pltpu.make_async_copy(
            result.at[:, j + 1, pl.ds(TOP, height), :],
            out.at[0, :, :, pl.ds(pl.multiple_of(j * LANES, LANES), LANES)],
            out_sem.at[j],
        )

    def strip(t, carry):
        start = t * stride + LANES - DEPTH
        a = start // LANES
        offset = start - a * LANES

        @pl.when((a < tiles) & ((t == 0) | ((start - stride) // LANES < a)))
        def _():
            await_tile(a)

        from_first = lane >= offset
        places = []
        for k in range(count):
            at = pl.ds(TOP - DEPTH + k, SUBS, stride=count)
            state = ()
            for f in range(fields):
                both = jnp.where(from_first, padded[f, a, at, :], padded[f, a + 1, at, :])
                state += (into[f] * pltpu.roll(both, LANES - offset, 1),)
            put_row(pred, k, state)
            places.append((pred_slope, k, state))
        put_slopes(matrix, places)

        @pl.when(level == 0)
        def _():
            lax.fori_loop(0, STEPS, lambda m, x: (predict(pred, pred_slope, matrix), x)[1], 0)

        @pl.when(level == 1)
        def _():
            first_step(pred, pred_slope, matrix, base)

            def middle(m, x):
                middle_step(pred, pred_slope, matrix, base, corr, corr_slope)
                return x

            lax.fori_loop(1, STEPS, middle, 0)
            last_step(pred, pred_slope, base)

        source = jnp.where(from_first, lane - offset, lane - offset + LANES)
        inside = (source >= DEPTH) & (source < DEPTH + stride)
        low, high = from_first & inside, jnp.logical_not(from_first) & inside
        for f in range(fields):
            for k in range(count):
                at = pl.ds(TOP - DEPTH + k, SUBS, stride=count)
                moved = pltpu.roll((1.0 / into[f]) * pred[f, k], offset, 1)
                result[f, a, at, :] = jnp.where(low, moved, result[f, a, at, :])
                result[f, a + 1, at, :] = jnp.where(high, moved, result[f, a + 1, at, :])
        done = jnp.minimum(tiles, (t + 1) * stride // LANES)
        before = jnp.minimum(tiles, t * stride // LANES)

        @pl.when(done > before)
        def _():
            out_copy(done - 1).start()

        return carry

    lax.fori_loop(0, strips, strip, 0)
    for j in range(tiles):
        out_copy(j).wait()


def call_window(initial, rows, nine, cols, diag):
    fields, height, width = initial.shape
    tiles = width // LANES
    count = -(-(height + 2 * DEPTH) // SUBS)
    padded_rows = height + 2 * TOP
    vmem = lambda *dims: pltpu.VMEM(dims, jnp.float32)
    anywhere = pl.BlockSpec(memory_space=pl.ANY)
    local = pl.BlockSpec(memory_space=pltpu.VMEM)
    return pl.pallas_call(
        window,
        out_shape=jax.ShapeDtypeStruct((1, fields, height, width), jnp.float32),
        in_specs=[anywhere, anywhere, local, local, local],
        out_specs=anywhere,
        scratch_shapes=[
            vmem(fields, tiles + 2, padded_rows, LANES),
            vmem(fields, tiles + 2, padded_rows, LANES),
            vmem(fields, count, SUBS, LANES),
            vmem(fields, count, SUBS, LANES),
            vmem(fields, count, SUBS, LANES),
            vmem(fields, count, SUBS, LANES),
            vmem(fields, count, SUBS, LANES),
            pltpu.VMEM((2 * LANES, LANES), jnp.bfloat16),
            pltpu.SemaphoreType.DMA((tiles,)),
            pltpu.SemaphoreType.DMA((2, tiles)),
            pltpu.SemaphoreType.DMA((tiles,)),
        ],
        compiler_params=pltpu.CompilerParams(vmem_limit_bytes=65994752),
        name="window",
    )(initial, rows, nine, cols, diag)


def body(initial):
    return call_window(initial, *call_exchange(initial))


def solution(mesh):
    return jax.shard_map(
        body,
        mesh=mesh,
        in_specs=(P(None, "row", "col"),),
        out_specs=P("level", None, "row", "col"),
        check_vma=False,
    )
```
